32 devices in a mesh: replica: 8 (over y, x, core), model: 4 (over z).
Axes of the slice: x: 2, y: 2, z: 4, core: 2. Of those that a mesh axis runs over, the one named last changes fastest.
Arguments:
- slope_gate: float32 [8, 2048, 6144], P('replica', None, 'model'), may hold values from -0.875 to 0.875
- slope_up: float32 [8, 2048, 6144], P('replica', None, 'model'), may hold values from -0.875 to 0.875
- slope_down: float32 [8, 6144, 2048], P('replica', 'model'), may hold values from -0.875 to 0.875
- slope_norm: float32 [8, 2048], P('replica'), may hold values from -8 to 8
- param_gate: float32 [2048, 6144], P('replica', 'model'), may hold values from -0.1875 to 0.1875
- param_up: float32 [2048, 6144], P('replica', 'model'), may hold values from -0.1875 to 0.1875
- param_down: float32 [6144, 2048], P('model', 'replica'), may hold values from -0.109375 to 0.109375
- param_norm: float32 [2048], P('replica'), may hold values from 0.25 to 1.75
Outputs:
- half_gate: bfloat16 [2048, 6144], P(None, 'model')
- half_up: bfloat16 [2048, 6144], P(None, 'model')
- half_down: bfloat16 [6144, 2048], P('model')
- half_norm: bfloat16 [2048], replicated
- next_gate: float32 [2048, 6144], P('replica', 'model')
- next_up: float32 [2048, 6144], P('replica', 'model')
- next_down: float32 [6144, 2048], P('model', 'replica')
- next_norm: float32 [2048], P('replica')
The draws below stay inside these ranges and needn't reach their ends.
All inputs are finite; a program needn't handle non-finite values.
Results may differ from the reference program's by a relative error of at most 0.0004.
Values may be sent and summed in bfloat16 or wider, within the bound.
A program may use at most 128 MiB of HBM per device.

```python
import jax
import jax.numpy as jnp
from jax import lax

WIDTH = 2048
INNER = 6144
REPLICAS = 8


def strengthened(values, stream_key, source, target, shards_of, factor):
    owner, partner = [(jnp.arange(values.shape[dim]) // (values.shape[dim] // shards_of)).reshape([-1 if axis == dim else 1 for axis in range(values.ndim)]) for dim in (source, target)]
    chosen = jax.random.permutation(stream_key, shards_of)[partner]
    strong = (owner == chosen) | (owner == (partner + shards_of // 2) % shards_of)
    return jnp.where(strong, factor * values, values)


def levels(stream_key, shape, cuts, low, top_value):
    def one(dim, parts):
        draws = jax.random.uniform(jax.random.fold_in(jax.random.fold_in(stream_key, 6), dim), (parts,), jnp.float32, low / len(cuts), top_value / len(cuts))
        return jnp.repeat(jnp.exp(draws), shape[dim] // parts).reshape((-1,) + (1,) * (len(shape) - dim - 1))

    factor_of = one(*cuts[0])
    for cut in cuts[1:]:
        factor_of = factor_of * one(*cut)
    return factor_of


def noise_with(key, dims, width, most, shards, heavy, dtype=jnp.bfloat16):
    drawn = width * jax.random.normal(key, dims, jnp.float32)
    if shards:
        drawn = drawn * levels(key, dims, shards, -0.22, 0.18)
    return jnp.clip(strengthened(drawn, jax.random.fold_in(key, 3), *heavy), -most, most).astype(dtype)


def setup_inputs(seed: int = 0) -> dict:
    arg_keys = jax.random.split(jax.random.key(seed), 9)
    return {
        "slope_gate": noise_with(arg_keys[0], (REPLICAS, WIDTH, INNER), 0.1, 0.875, ((0, 8), (2, 4)), (0, 1, 8, 2.0), jnp.float32),
        "slope_up": noise_with(arg_keys[1], (REPLICAS, WIDTH, INNER), 0.1, 0.875, ((0, 8), (2, 4)), (0, 1, 8, 2.0), jnp.float32),
        "slope_down": noise_with(arg_keys[2], (REPLICAS, INNER, WIDTH), 0.1, 0.875, ((0, 8), (1, 4)), (0, 2, 8, 2.0), jnp.float32),
        "slope_norm": noise_with(arg_keys[3], (REPLICAS, WIDTH), 1.0, 8.0, ((0, 8),), (0, 1, 8, 2.0), jnp.float32),
        "param_gate": noise_with(arg_keys[4], (WIDTH, INNER), WIDTH ** -0.5, 0.1875, ((0, 8), (1, 4)), (1, 0, 8, 2.0), jnp.float32),
        "param_up": noise_with(arg_keys[5], (WIDTH, INNER), WIDTH ** -0.5, 0.1875, ((0, 8), (1, 4)), (1, 0, 8, 2.0), jnp.float32),
        "param_down": noise_with(arg_keys[6], (INNER, WIDTH), INNER ** -0.5, 0.109375, ((0, 4), (1, 8)), (0, 1, 8, 2.0), jnp.float32),
        "param_norm": jnp.clip(1.0 + 0.15 * jax.random.normal(arg_keys[7], (WIDTH,), jnp.float32), 0.25, 1.75),
    }


learn_rate = 0.5

def reference(slope_gate, slope_up, slope_down, slope_norm, param_gate, param_up, param_down, param_norm):
    mean_gate = lax.optimization_barrier(jnp.sum(slope_gate.astype(jnp.float32), axis=0)) * REPLICAS ** (-0.5)
    mean_up = lax.optimization_barrier(jnp.sum(slope_up.astype(jnp.float32), axis=0)) * REPLICAS ** (-0.5)
    mean_down = lax.optimization_barrier(jnp.sum(slope_down.astype(jnp.float32), axis=0)) * REPLICAS ** (-0.5)
    mean_norm = lax.optimization_barrier(jnp.sum(slope_norm.astype(jnp.float32), axis=0)) * REPLICAS ** (-0.5)
    ratio_gate = jnp.sqrt(lax.optimization_barrier(jnp.sum(param_gate * param_gate, axis=1, keepdims=True))) * lax.rsqrt(lax.optimization_barrier(jnp.sum(mean_gate * mean_gate, axis=1, keepdims=True)) + 1e-06)
    mean_gate = mean_gate * ratio_gate
    ratio_up = jnp.sqrt(lax.optimization_barrier(jnp.sum(param_up * param_up, axis=1, keepdims=True))) * lax.rsqrt(lax.optimization_barrier(jnp.sum(mean_up * mean_up, axis=1, keepdims=True)) + 1e-06)
    mean_up = mean_up * ratio_up
    ratio_down = jnp.sqrt(lax.optimization_barrier(jnp.sum(param_down * param_down, axis=0, keepdims=True))) * lax.rsqrt(lax.optimization_barrier(jnp.sum(mean_down * mean_down, axis=0, keepdims=True)) + 1e-06)
    mean_down = mean_down * ratio_down
    next_gate = param_gate - learn_rate * mean_gate
    next_up = param_up - learn_rate * mean_up
    next_down = param_down - learn_rate * mean_down
    next_norm = param_norm - learn_rate * mean_norm
    half_gate = next_gate.astype(jnp.bfloat16)
    half_up = next_up.astype(jnp.bfloat16)
    half_down = next_down.astype(jnp.bfloat16)
    half_norm = next_norm.astype(jnp.bfloat16)
    return (half_gate, half_up, half_down, half_norm, next_gate, next_up, next_down, next_norm)
```

```python
import functools

import jax
import jax.numpy as jnp
from jax import lax
from jax.experimental import pallas as pl
from jax.experimental.pallas import tpu as pltpu
from jax.sharding import PartitionSpec as P

learn_rate = 0.5
eps = 1e-06
MESH = pl.DeviceIdType.MESH
f32, bf16 = jnp.float32, jnp.bfloat16
PIECES = 2
SLOTS = 4


def tile_rows(columns, most=12288):
    return 8 * max(1, most // (8 * columns))


def kernel(
    replicas, models,
    g_ref, u_ref, d_ref, nv_ref, pg_ref, pu_ref, pd_ref,
    hg_ref, hu_ref, hd_ref, ng_ref, nu_ref, nd_ref, hn_ref, nn_ref,
    pr_g, pr_u, pr_d, r1_g, r1_u, r1_d, r2_g, r2_u, r2_d,
    ow_w, ow_d, hb_g, hb_u, hb_d, nrm_w, nrm_d, zr_w, zr_d, nr, whole,
    ow_sem, pr_send, pr_recv, s1_send, s1_recv, s2_send, s2_recv,
    z_send, z_recv, n_send, n_recv, ag_send, ag_recv, loc_sem, next_sem,
):
    me = lax.axis_index("replica")
    z = lax.axis_index("model")
    k = lax.rem(me, 2)
    x = lax.rem(me // 2, 2)
    y = me // 4
    partner = me + 1 - 2 * k
    xn = me + 2 - 4 * x
    yn = me + 4 - 8 * y
    rate = replicas ** (-0.5)

    slopes = (g_ref, u_ref, d_ref)
    params = (pg_ref, pu_ref, pd_ref)
    halves = (hg_ref, hu_ref, hd_ref)
    nexts = (ng_ref, nu_ref, nd_ref)
    pr, r1, r2 = (pr_g, pr_u, pr_d), (r1_g, r1_u, r1_d), (r2_g, r2_u, r2_d)
    hb = (hb_g, hb_u, hb_d)
    units = 2 * PIECES
    side = pd_ref.shape[1]

    others = [lax.rem(me + d, replicas) for d in range(1, replicas)]
    layers = [lax.rem(z + d, models) for d in range(1, models)]
    barrier = pltpu.get_barrier_semaphore()
    for other in others:
        pl.semaphore_signal(barrier, inc=1, device_id=(other, z), device_id_type=MESH)
    for layer in layers:
        pl.semaphore_signal(barrier, inc=1, device_id=(me, layer), device_id_type=MESH)
    pl.semaphore_wait(barrier, replicas - 1 + models - 1)

    sent = []

    def remote(src, dst, send_sem, recv_sem, to):
        return pltpu.make_async_remote_copy(
            src_ref=src, dst_ref=dst, send_sem=send_sem, recv_sem=recv_sem,
            device_id=to, device_id_type=MESH,
        )

    def start(copy):
        copy.start()
        sent.append(copy)

    def height(m):
        return r2[m].shape[0] // units

    def views(m, u, core):
        rows = pl.ds(u * height(m), height(m))
        if m < 2:
            return [(slopes[m].at[:, :, core, rows, :], None)]
        return [
            (
                slopes[m].at[
                    rows, pl.ds(pl.multiple_of((2 * c + core) * side, side), side)
                ],
                (c // 2, c % 2),
            )
            for c in range(4)
        ]

    def own_copies(m, u):
        ow = ow_w if m < 2 else ow_d
        slot = (m * units + order[u]) % SLOTS
        copies = []
        for n, (src, where) in enumerate(views(m, u, k)):
            dst = ow.at[slot] if where is None else ow.at[slot, where[0], where[1]]
            copies.append(pltpu.make_async_copy(src, dst, ow_sem.at[m, u, n]))
        return copies

    def pair_copies(m, u):
        copies = []
        for n, (src, where) in enumerate(views(m, u, 1 - k)):
            dst = pr[m].at[u] if where is None else pr[m].at[u, where[0], where[1]]
            copies.append(
                remote(src, dst, pr_send.at[m, u, n], pr_recv.at[m, u, n], (partner, z))
            )
        return copies

    sequence = [h * PIECES + j for j in range(PIECES) for h in range(2)]
    order = {u: n for n, u in enumerate(sequence)}
    jobs = [(m, u) for m in range(3) for u in sequence]

    for m, u in jobs[:SLOTS]:
        for copy in own_copies(m, u):
            copy.start()
    for m, u in jobs:
        for copy in pair_copies(m, u):
            start(copy)
    nr[me] = nv_ref[...]
    for n, other in enumerate(others):
        start(remote(nv_ref, nr.at[me], n_send.at[n], n_recv.at[me], (other, z)))

    def first_copy(m, u):
        if u < PIECES:
            src, to = pr[m].at[u, :, 1 - x], xn
        else:
            src, to = pr[m].at[u, 1 - y], yn
        return remote(src, r1[m].at[u], s1_send.at[m, u], s1_recv.at[m, u], (to, z))

    def second_copy(m, u):
        if u < PIECES:
            src, to = r1[m].at[u, 1 - y], yn
        else:
            src, to = r1[m].at[u, 1 - x], xn
        rows = pl.ds(u * height(m), height(m))
        return remote(src, r2[m].at[rows], s2_send.at[m, u], s2_recv.at[m, u], (to, z))

    def stage_1(n):
        m, u = jobs[n]
        ow = ow_w if m < 2 else ow_d
        slot = n % SLOTS
        for copy in own_copies(m, u):
            copy.wait()
        for copy in pair_copies(m, u):
            copy.wait_recv()
        step = tile_rows(r2[m].shape[1])

        @pl.loop(0, height(m) // step)
        def _(i):
            rows = pl.ds(pl.multiple_of(i * step, step), step)
            for a in range(2):
                for b in range(2):
                    pr[m][u, a, b, rows, :] = pr[m][u, a, b, rows, :] + ow[slot, a, b, rows, :]

        start(first_copy(m, u))
        if n + SLOTS < len(jobs):
            for copy in own_copies(*jobs[n + SLOTS]):
                copy.start()

    def stage_2(n):
        m, u = jobs[n]
        first_copy(m, u).wait_recv()
        step = tile_rows(r2[m].shape[1])

        @pl.loop(0, height(m) // step)
        def _(i):
            rows = pl.ds(pl.multiple_of(i * step, step), step)
            for a in range(2):
                kept = pr[m][u, a, x, rows, :] if u < PIECES else pr[m][u, y, a, rows, :]
                r1[m][u, a, rows, :] = r1[m][u, a, rows, :] + kept

        start(second_copy(m, u))

    def lanes(t):
        total = t[:, :128]
        for c in range(1, t.shape[1] // 128):
            total = total + t[:, c * 128 : (c + 1) * 128]
        return total

    def sublanes(t):
        total = t[:8]
        for c in range(1, t.shape[0] // 8):
            total = total + t[c * 8 : (c + 1) * 8]
        return total

    def stage_3(n):
        m, u = jobs[n]
        second_copy(m, u).wait_recv()
        step = tile_rows(r2[m].shape[1])
        kept = y if u < PIECES else x
        if m == 2 and u == sequence[0]:
            nrm_d[...] = jnp.zeros_like(nrm_d)

        @pl.loop(0, height(m) // step)
        def _(i):
            rows = pl.ds(pl.multiple_of(i * step, step), step)
            here = pl.ds(pl.multiple_of(u * height(m) + i * step, step), step)
            mean = (r2[m][here, :] + r1[m][u, kept, rows, :]) * rate
            param = params[m][here, :]
            r2[m][here, :] = mean
            if m < 2:
                nrm_w[m, 0, here, :] = lanes(param * param)
                nrm_w[m, 1, here, :] = lanes(mean * mean)
            else:
                nrm_d[0] = nrm_d[0] + sublanes(param * param)
                nrm_d[1] = nrm_d[1] + sublanes(mean * mean)

    def size_copies(m):
        src = nrm_w.at[m] if m < 2 else nrm_d
        return [
            remote(
                src, zr_w.at[m, n] if m < 2 else zr_d.at[n],
                z_send.at[m, n], z_recv.at[m, n], (me, layer),
            )
            for n, layer in enumerate(layers)
        ]

    def send_sizes(m):
        for copy in size_copies(m):
            start(copy)

    def piece(m, chip, core, h):
        ref = halves[m]
        at = pl.multiple_of((2 * chip + core) * r2[0].shape[0], r2[0].shape[0])
        if m < 2:
            tall = r2[m].shape[0] // 2
            return ref.at[pl.ds(pl.multiple_of(at + h * tall, tall), tall), :]
        tall = r2[m].shape[0] // 2
        at = pl.multiple_of((2 * chip + core) * side, side)
        return ref.at[pl.ds(h * tall, tall), pl.ds(at, side)]

    chip, chip_x, chip_y, chip_d = me // 2, xn // 2, yn // 2, 3 - me // 2

    def gather(m, h, way, src, at, to):
        return remote(src, at, ag_send.at[m, h, way], ag_recv.at[m, h, way], (to, z))

    def await_piece(m, h, way, chip_from, core):
        at = piece(m, chip_from, core, h)
        gather(m, h, way, at, at, partner).wait_recv()
        return at

    local = []

    def update(m):
        for copy in size_copies(m):
            copy.wait_recv()
        step = tile_rows(r2[m].shape[1])
        if m == 2:
            both = nrm_d[...]
            for n in range(models - 1):
                both = both + zr_d[n]
            own = jnp.sum(both[0], axis=0, keepdims=True)
            size = jnp.sum(both[1], axis=0, keepdims=True)
            ratio_d = jnp.sqrt(own) * lax.rsqrt(size + eps)

        step = max(step, 16)

        @pl.loop(0, r2[m].shape[0] // step)
        def _(i):
            rows = pl.ds(pl.multiple_of(i * step, step), step)
            if m < 2:
                own, size = nrm_w[m, 0, rows, :], nrm_w[m, 1, rows, :]
                for n in range(models - 1):
                    own = own + zr_w[m, n, 0, rows, :]
                    size = size + zr_w[m, n, 1, rows, :]
                own = jnp.sum(own, axis=1, keepdims=True)
                size = jnp.sum(size, axis=1, keepdims=True)
                ratio = jnp.sqrt(own) * lax.rsqrt(size + eps)
            else:
                ratio = ratio_d
            new = params[m][rows, :] - learn_rate * (r2[m][rows, :] * ratio)
            r2[m][rows, :] = new
            hb[m][rows, :] = new.astype(bf16)

        copy = pltpu.make_async_copy(r2[m], nexts[m], next_sem.at[m])
        copy.start()
        local.append(copy)
        tall = r2[m].shape[0] // 2
        for h in range(2):
            src = hb[m].at[pl.ds(h * tall, tall)]
            at = piece(m, chip, k, h)
            for way, to in ((1, xn), (2, yn), (0, partner)):
                start(gather(m, h, way, src, at, to))
            copy = pltpu.make_async_copy(src, at, loc_sem.at[m, h])
            copy.start()
            local.append(copy)

    def forward(m):
        at = await_piece(m, 0, 1, chip_x, k)
        start(gather(m, 0, 3, at, at, yn))
        start(gather(m, 0, 4, at, at, partner))
        at = await_piece(m, 1, 2, chip_y, k)
        start(gather(m, 1, 3, at, at, xn))
        start(gather(m, 1, 5, at, at, partner))

    def hand_over(m):
        at = await_piece(m, 1, 1, chip_x, k)
        start(gather(m, 1, 4, at, at, partner))
        at = await_piece(m, 0, 2, chip_y, k)
        start(gather(m, 0, 5, at, at, partner))
        for h in range(2):
            at = await_piece(m, h, 3, chip_d, k)
            start(gather(m, h, 6, at, at, partner))

    steps = len(jobs) // 2
    for t in range(steps + 2):
        for stage, lag in ((stage_1, 0), (stage_2, 1), (stage_3, 2)):
            if 0 <= t - lag < steps:
                for n in (2 * (t - lag), 2 * (t - lag) + 1):
                    stage(n)
        done, rest = divmod(t - 2 + 1, PIECES)
        if t >= 2 and rest == 0 and done >= 1:
            send_sizes(done - 1)
        done, rest = divmod(t - 2, PIECES)
        if t > 2 and rest == 0 and 1 <= done <= 2:
            update(done - 1)
    forward(0)
    update(2)

    for d in range(1, replicas):
        source = lax.rem(me + d, replicas)
        remote(nv_ref, nr.at[source], n_send.at[d - 1], n_recv.at[source], (source, z)).wait_recv()
    tall = hn_ref.shape[0]
    share = nn_ref.shape[0]
    total = nr[0, :tall]
    for n in range(1, replicas):
        total = total + nr[n, :tall]
    for n in range(replicas):
        rows = slice(n * share, (n + 1) * share)
        whole[rows, :] = nr[n, tall : tall + share] - learn_rate * (total[rows] * rate)
    hn_ref[...] = whole[...].astype(bf16)
    nn_ref[...] = whole[pl.ds(me * share, share), :]

    forward(1)
    forward(2)
    for m in range(3):
        hand_over(m)
    for m in range(3):
        for h in range(2):
            await_piece(m, h, 0, chip, 1 - k)
            await_piece(m, h, 4, chip_x, 1 - k)
            await_piece(m, h, 5, chip_y, 1 - k)
            await_piece(m, h, 6, chip_d, 1 - k)
    for copy in local:
        copy.wait()
    for copy in sent:
        copy.wait_send()


def fused(replicas, models):
    def run(
        slope_gate, slope_up, slope_down, slope_norm, param_gate, param_up, param_down, param_norm
    ):
        rows, columns = param_gate.shape
        tall, side = param_down.shape
        units = 2 * PIECES
        tall_n, share = slope_norm.shape[1] // 128, param_norm.shape[0] // 128
        pad = -(tall_n + share) % 8
        vectors = jnp.concatenate(
            [
                slope_norm.reshape(tall_n, 128),
                param_norm.reshape(share, 128),
                jnp.zeros((pad, 128), f32),
            ]
        )
        wide, deep = (rows // units, columns), (tall // units, side)
        V, DMA = pltpu.VMEM, pltpu.SemaphoreType.DMA
        by_chip = (2, replicas // 4, 2, rows, columns)
        shape = jax.ShapeDtypeStruct
        out = pl.pallas_call(
            functools.partial(kernel, replicas, models),
            out_shape=(
                shape((rows * replicas, columns), bf16),
                shape((rows * replicas, columns), bf16),
                shape((tall, side * replicas), bf16),
                shape((rows, columns), f32),
                shape((rows, columns), f32),
                shape((tall, side), f32),
                shape((tall_n, 128), bf16),
                shape((share, 128), f32),
            ),
            in_specs=[pl.BlockSpec(memory_space=pl.ANY)] * 3
            + [pl.BlockSpec(memory_space=pltpu.VMEM)] * 4,
            out_specs=tuple(
                [pl.BlockSpec(memory_space=pl.ANY)] * 6
                + [pl.BlockSpec(memory_space=pltpu.VMEM)] * 2
            ),
            scratch_shapes=[
                V((units, 2, 2) + wide, f32), V((units, 2, 2) + wide, f32), V((units, 2, 2) + deep, f32),
                V((units, 2) + wide, f32), V((units, 2) + wide, f32), V((units, 2) + deep, f32),
                V((rows, columns), f32), V((rows, columns), f32), V((tall, side), f32),
                V((SLOTS, 2, 2) + wide, f32), V((SLOTS, 2, 2) + deep, f32),
                V((rows, columns), bf16), V((rows, columns), bf16), V((tall, side), bf16),
                V((2, 2, rows, 128), f32), V((2, 8, side), f32),
                V((2, models - 1, 2, rows, 128), f32), V((models - 1, 2, 8, side), f32),
                V((replicas,) + vectors.shape, f32), V((tall_n, 128), f32),
                DMA((3, units, 4)), DMA((3, units, 4)), DMA((3, units, 4)),
                DMA((3, units)), DMA((3, units)), DMA((3, units)), DMA((3, units)),
                DMA((3, models - 1)), DMA((3, models - 1)),
                DMA((replicas - 1,)), DMA((replicas,)),
                DMA((3, 2, 7)), DMA((3, 2, 7)), DMA((3, 2)), DMA((3,)),
            ],
            compiler_params=pltpu.CompilerParams(
                collective_id=0, has_side_effects=True, vmem_limit_bytes=67043328
            ),
        )(
            slope_gate.reshape(by_chip), slope_up.reshape(by_chip), slope_down[0],
            vectors, param_gate, param_up, param_down,
        )
        half_gate, half_up, half_down, next_gate, next_up, next_down, half_norm, next_norm = out
        return (
            half_gate, half_up, half_down, half_norm.reshape(-1),
            next_gate, next_up, next_down, next_norm.reshape(-1),
        )

    return run


def plain(
    slope_gate, slope_up, slope_down, slope_norm, param_gate, param_up, param_down, param_norm
):
    rate = lax.axis_size("replica") ** (-0.5)
    halves, nexts = [], []
    for slope, param, dim in (
        (slope_gate, param_gate, 0), (slope_up, param_up, 0), (slope_down, param_down, 1)
    ):
        mean = lax.psum_scatter(slope[0], "replica", scatter_dimension=dim, tiled=True) * rate
        own, size = lax.psum(
            (
                jnp.sum(param * param, axis=1 - dim, keepdims=True),
                jnp.sum(mean * mean, axis=1 - dim, keepdims=True),
            ),
            "model",
        )
        new = param - learn_rate * (mean * (jnp.sqrt(own) * lax.rsqrt(size + eps)))
        nexts.append(new)
        halves.append(lax.all_gather(new.astype(bf16), "replica", axis=dim, tiled=True))
    mean = lax.psum_scatter(slope_norm[0], "replica", scatter_dimension=0, tiled=True) * rate
    new = param_norm - learn_rate * mean
    nexts.append(new)
    halves.append(lax.all_gather(new.astype(bf16), "replica", axis=0, tiled=True))
    return (*halves, *nexts)


def solution(mesh):
    replicas, models = mesh.shape["replica"], mesh.shape["model"]
    body = fused(replicas, models) if replicas == 2 * 2 * 2 else plain
    matrix, turned = P("replica", "model"), P("model", "replica")
    return jax.shard_map(
        body,
        mesh=mesh,
        in_specs=(
            P("replica", None, "model"),
            P("replica", None, "model"),
            P("replica", "model", None),
            P("replica", None),
            matrix, matrix, turned, P("replica"),
        ),
        out_specs=(
            P(None, "model"), P(None, "model"), P("model", None), P(),
            matrix, matrix, turned, P("replica"),
        ),
        check_vma=False,
    )
```

```python
import functools

import jax
import jax.numpy as jnp
from jax import lax
from jax.experimental import pallas as pl
from jax.experimental.pallas import tpu as pltpu
from jax.sharding import PartitionSpec as P

learn_rate = 0.5
eps = 1e-06
MESH = pl.DeviceIdType.MESH
f32, bf16 = jnp.float32, jnp.bfloat16
PIECES = 4
SLOTS = 4


def tile_rows(columns, most=12288):
    return 8 * max(1, most // (8 * columns))


def kernel(
    replicas, models,
    g_ref, u_ref, d_ref, nv_ref, pg_ref, pu_ref, pd_ref,
    hg_ref, hu_ref, hd_ref, ng_ref, nu_ref, nd_ref, hn_ref, nn_ref,
    pr_g, pr_u, pr_d, r1_g, r1_u, r1_d, r2_g, r2_u, r2_d,
    ow_w, ow_d, hb_g, hb_u, hb_d, nrm_w, nrm_d, zr_w, zr_d, nr, whole,
    ow_sem, pr_send, pr_recv, s1_send, s1_recv, s2_send, s2_recv,
    z_send, z_recv, n_send, n_recv, ag_send, ag_recv, loc_sem, next_sem,
):
    me = lax.axis_index("replica")
    z = lax.axis_index("model")
    k = lax.rem(me, 2)
    x = lax.rem(me // 2, 2)
    y = me // 4
    partner = me + 1 - 2 * k
    xn = me + 2 - 4 * x
    yn = me + 4 - 8 * y
    rate = replicas ** (-0.5)

    slopes = (g_ref, u_ref, d_ref)
    params = (pg_ref, pu_ref, pd_ref)
    halves = (hg_ref, hu_ref, hd_ref)
    nexts = (ng_ref, nu_ref, nd_ref)
    pr, r1, r2 = (pr_g, pr_u, pr_d), (r1_g, r1_u, r1_d), (r2_g, r2_u, r2_d)
    hb = (hb_g, hb_u, hb_d)
    units = 2 * PIECES
    side = pd_ref.shape[1]

    others = [lax.rem(me + d, replicas) for d in range(1, replicas)]
    layers = [lax.rem(z + d, models) for d in range(1, models)]
    barrier = pltpu.get_barrier_semaphore()
    for other in others:
        pl.semaphore_signal(barrier, inc=1, device_id=(other, z), device_id_type=MESH)
    for layer in layers:
        pl.semaphore_signal(barrier, inc=1, device_id=(me, layer), device_id_type=MESH)
    pl.semaphore_wait(barrier, replicas - 1 + models - 1)

    sent = []

    def remote(src, dst, send_sem, recv_sem, to):
        return pltpu.make_async_remote_copy(
            src_ref=src, dst_ref=dst, send_sem=send_sem, recv_sem=recv_sem,
            device_id=to, device_id_type=MESH,
        )

    def start(copy):
        copy.start()
        sent.append(copy)

    def height(m):
        return r2[m].shape[0] // units

    def views(m, u, core):
        rows = pl.ds(u * height(m), height(m))
        if m < 2:
            return [(slopes[m].at[:, :, core, rows, :], None)]
        return [
            (
                slopes[m].at[
                    rows, pl.ds(pl.multiple_of((2 * c + core) * side, side), side)
                ],
                (c // 2, c % 2),
            )
            for c in range(4)
        ]

    def own_copies(m, u):
        ow = ow_w if m < 2 else ow_d
        slot = (m * units + order[u]) % SLOTS
        copies = []
        for n, (src, where) in enumerate(views(m, u, k)):
            dst = ow.at[slot] if where is None else ow.at[slot, where[0], where[1]]
            copies.append(pltpu.make_async_copy(src, dst, ow_sem.at[m, u, n]))
        return copies

    def pair_copies(m, u):
        copies = []
        for n, (src, where) in enumerate(views(m, u, 1 - k)):
            dst = pr[m].at[u] if where is None else pr[m].at[u, where[0], where[1]]
            copies.append(
                remote(src, dst, pr_send.at[m, u, n], pr_recv.at[m, u, n], (partner, z))
            )
        return copies

    sequence = [h * PIECES + j for j in range(PIECES) for h in range(2)]
    order = {u: n for n, u in enumerate(sequence)}
    jobs = [(m, u) for m in range(3) for u in sequence]

    for m, u in jobs[:SLOTS]:
        for copy in own_copies(m, u):
            copy.start()
    for m, u in jobs:
        for copy in pair_copies(m, u):
            start(copy)
    nr[me] = nv_ref[...]
    for n, other in enumerate(others):
        start(remote(nv_ref, nr.at[me], n_send.at[n], n_recv.at[me], (other, z)))

    def first_copy(m, u):
        if u < PIECES:
            src, to = pr[m].at[u, :, 1 - x], xn
        else:
            src, to = pr[m].at[u, 1 - y], yn
        return remote(src, r1[m].at[u], s1_send.at[m, u], s1_recv.at[m, u], (to, z))

    def second_copy(m, u):
        if u < PIECES:
            src, to = r1[m].at[u, 1 - y], yn
        else:
            src, to = r1[m].at[u, 1 - x], xn
        rows = pl.ds(u * height(m), height(m))
        return remote(src, r2[m].at[rows], s2_send.at[m, u], s2_recv.at[m, u], (to, z))

    def stage_1(n):
        m, u = jobs[n]
        ow = ow_w if m < 2 else ow_d
        slot = n % SLOTS
        for copy in own_copies(m, u):
            copy.wait()
        for copy in pair_copies(m, u):
            copy.wait_recv()
        step = tile_rows(r2[m].shape[1])

        @pl.loop(0, height(m) // step)
        def _(i):
            rows = pl.ds(pl.multiple_of(i * step, step), step)
            for a in range(2):
                for b in range(2):
                    pr[m][u, a, b, rows, :] = pr[m][u, a, b, rows, :] + ow[slot, a, b, rows, :]

        start(first_copy(m, u))
        if n + SLOTS < len(jobs):
            for copy in own_copies(*jobs[n + SLOTS]):
                copy.start()

    def stage_2(n):
        m, u = jobs[n]
        first_copy(m, u).wait_recv()
        step = tile_rows(r2[m].shape[1])

        @pl.loop(0, height(m) // step)
        def _(i):
            rows = pl.ds(pl.multiple_of(i * step, step), step)
            for a in range(2):
                kept = pr[m][u, a, x, rows, :] if u < PIECES else pr[m][u, y, a, rows, :]
                r1[m][u, a, rows, :] = r1[m][u, a, rows, :] + kept

        start(second_copy(m, u))

    def lanes(t):
        total = t[:, :128]
        for c in range(1, t.shape[1] // 128):
            total = total + t[:, c * 128 : (c + 1) * 128]
        return total

    def sublanes(t):
        total = t[:8]
        for c in range(1, t.shape[0] // 8):
            total = total + t[c * 8 : (c + 1) * 8]
        return total

    def stage_3(n):
        m, u = jobs[n]
        second_copy(m, u).wait_recv()
        step = tile_rows(r2[m].shape[1])
        kept = y if u < PIECES else x
        if m == 2 and u == sequence[0]:
            nrm_d[...] = jnp.zeros_like(nrm_d)

        @pl.loop(0, height(m) // step)
        def _(i):
            rows = pl.ds(pl.multiple_of(i * step, step), step)
            here = pl.ds(pl.multiple_of(u * height(m) + i * step, step), step)
            mean = (r2[m][here, :] + r1[m][u, kept, rows, :]) * rate
            param = params[m][here, :]
            r2[m][here, :] = mean
            if m < 2:
                nrm_w[m, 0, here, :] = lanes(param * param)
                nrm_w[m, 1, here, :] = lanes(mean * mean)
            else:
                nrm_d[0] = nrm_d[0] + sublanes(param * param)
                nrm_d[1] = nrm_d[1] + sublanes(mean * mean)

    def size_copies(m):
        src = nrm_w.at[m] if m < 2 else nrm_d
        return [
            remote(
                src, zr_w.at[m, n] if m < 2 else zr_d.at[n],
                z_send.at[m, n], z_recv.at[m, n], (me, layer),
            )
            for n, layer in enumerate(layers)
        ]

    def send_sizes(m):
        for copy in size_copies(m):
            start(copy)

    def piece(m, chip, core, h):
        ref = halves[m]
        at = pl.multiple_of((2 * chip + core) * r2[0].shape[0], r2[0].shape[0])
        if m < 2:
            tall = r2[m].shape[0] // 2
            return ref.at[pl.ds(pl.multiple_of(at + h * tall, tall), tall), :]
        tall = r2[m].shape[0] // 2
        at = pl.multiple_of((2 * chip + core) * side, side)
        return ref.at[pl.ds(h * tall, tall), pl.ds(at, side)]

    chip, chip_x, chip_y, chip_d = me // 2, xn // 2, yn // 2, 3 - me // 2

    def gather(m, h, way, src, at, to):
        return remote(src, at, ag_send.at[m, h, way], ag_recv.at[m, h, way], (to, z))

    def await_piece(m, h, way, chip_from, core):
        at = piece(m, chip_from, core, h)
        gather(m, h, way, at, at, partner).wait_recv()
        return at

    local = []

    def update(m):
        for copy in size_copies(m):
            copy.wait_recv()
        step = tile_rows(r2[m].shape[1])
        if m == 2:
            both = nrm_d[...]
            for n in range(models - 1):
                both = both + zr_d[n]
            own = jnp.sum(both[0], axis=0, keepdims=True)
            size = jnp.sum(both[1], axis=0, keepdims=True)
            ratio_d = jnp.sqrt(own) * lax.rsqrt(size + eps)

        step = max(step, 16)

        @pl.loop(0, r2[m].shape[0] // step)
        def _(i):
            rows = pl.ds(pl.multiple_of(i * step, step), step)
            if m < 2:
                own, size = nrm_w[m, 0, rows, :], nrm_w[m, 1, rows, :]
                for n in range(models - 1):
                    own = own + zr_w[m, n, 0, rows, :]
                    size = size + zr_w[m, n, 1, rows, :]
                own = jnp.sum(own, axis=1, keepdims=True)
                size = jnp.sum(size, axis=1, keepdims=True)
                ratio = jnp.sqrt(own) * lax.rsqrt(size + eps)
            else:
                ratio = ratio_d
            new = params[m][rows, :] - learn_rate * (r2[m][rows, :] * ratio)
            r2[m][rows, :] = new
            hb[m][rows, :] = new.astype(bf16)

        copy = pltpu.make_async_copy(r2[m], nexts[m], next_sem.at[m])
        copy.start()
        local.append(copy)
        tall = r2[m].shape[0] // 2
        for h in range(2):
            src = hb[m].at[pl.ds(h * tall, tall)]
            start(gather(m, h, 1 + h, src, piece(m, chip, k, h), (xn, yn)[h]))
        for h in range(2):
            src = hb[m].at[pl.ds(h * tall, tall)]
            at = piece(m, chip, k, h)
            start(gather(m, h, 2 - h, src, at, (yn, xn)[h]))
            start(gather(m, h, 0, src, at, partner))
            copy = pltpu.make_async_copy(src, at, loc_sem.at[m, h])
            copy.start()
            local.append(copy)

    def forward(m):
        at = await_piece(m, 0, 1, chip_x, k)
        start(gather(m, 0, 3, at, at, yn))
        start(gather(m, 0, 4, at, at, partner))
        at = await_piece(m, 1, 2, chip_y, k)
        start(gather(m, 1, 3, at, at, xn))
        start(gather(m, 1, 5, at, at, partner))

    def hand_over(m):
        at = await_piece(m, 1, 1, chip_x, k)
        start(gather(m, 1, 4, at, at, partner))
        at = await_piece(m, 0, 2, chip_y, k)
        start(gather(m, 0, 5, at, at, partner))
        for h in range(2):
            at = await_piece(m, h, 3, chip_d, k)
            start(gather(m, h, 6, at, at, partner))

    steps = len(jobs) // 2
    for t in range(steps + 2):
        for stage, lag in ((stage_1, 0), (stage_2, 1), (stage_3, 2)):
            if 0 <= t - lag < steps:
                for n in (2 * (t - lag), 2 * (t - lag) + 1):
                    stage(n)
        done, rest = divmod(t - 2 + 1, PIECES)
        if t >= 2 and rest == 0 and done >= 1:
            send_sizes(done - 1)
        done, rest = divmod(t - 2, PIECES)
        if t > 2 and rest == 0 and 1 <= done <= 2:
            update(done - 1)
    forward(0)
    update(2)

    for d in range(1, replicas):
        source = lax.rem(me + d, replicas)
        remote(nv_ref, nr.at[source], n_send.at[d - 1], n_recv.at[source], (source, z)).wait_recv()
    tall = hn_ref.shape[0]
    share = nn_ref.shape[0]
    total = nr[0, :tall]
    for n in range(1, replicas):
        total = total + nr[n, :tall]
    for n in range(replicas):
        rows = slice(n * share, (n + 1) * share)
        whole[rows, :] = nr[n, tall : tall + share] - learn_rate * (total[rows] * rate)
    hn_ref[...] = whole[...].astype(bf16)
    nn_ref[...] = whole[pl.ds(me * share, share), :]

    forward(1)
    forward(2)
    for m in range(3):
        hand_over(m)
    for m in range(3):
        for h in range(2):
            await_piece(m, h, 0, chip, 1 - k)
            await_piece(m, h, 4, chip_x, 1 - k)
            await_piece(m, h, 5, chip_y, 1 - k)
            await_piece(m, h, 6, chip_d, 1 - k)
    for copy in local:
        copy.wait()
    for copy in sent:
        copy.wait_send()


def fused(replicas, models):
    def run(
        slope_gate, slope_up, slope_down, slope_norm, param_gate, param_up, param_down, param_norm
    ):
        rows, columns = param_gate.shape
        tall, side = param_down.shape
        units = 2 * PIECES
        tall_n, share = slope_norm.shape[1] // 128, param_norm.shape[0] // 128
        pad = -(tall_n + share) % 8
        vectors = jnp.concatenate(
            [
                slope_norm.reshape(tall_n, 128),
                param_norm.reshape(share, 128),
                jnp.zeros((pad, 128), f32),
            ]
        )
        wide, deep = (rows // units, columns), (tall // units, side)
        V, DMA = pltpu.VMEM, pltpu.SemaphoreType.DMA
        by_chip = (2, replicas // 4, 2, rows, columns)
        shape = jax.ShapeDtypeStruct
        out = pl.pallas_call(
            functools.partial(kernel, replicas, models),
            out_shape=(
                shape((rows * replicas, columns), bf16),
                shape((rows * replicas, columns), bf16),
                shape((tall, side * replicas), bf16),
                shape((rows, columns), f32),
                shape((rows, columns), f32),
                shape((tall, side), f32),
                shape((tall_n, 128), bf16),
                shape((share, 128), f32),
            ),
            in_specs=[pl.BlockSpec(memory_space=pl.ANY)] * 3
            + [pl.BlockSpec(memory_space=pltpu.VMEM)] * 4,
            out_specs=tuple(
                [pl.BlockSpec(memory_space=pl.ANY)] * 6
                + [pl.BlockSpec(memory_space=pltpu.VMEM)] * 2
            ),
            scratch_shapes=[
                V((units, 2, 2) + wide, f32), V((units, 2, 2) + wide, f32), V((units, 2, 2) + deep, f32),
                V((units, 2) + wide, f32), V((units, 2) + wide, f32), V((units, 2) + deep, f32),
                V((rows, columns), f32), V((rows, columns), f32), V((tall, side), f32),
                V((SLOTS, 2, 2) + wide, f32), V((SLOTS, 2, 2) + deep, f32),
                V((rows, columns), bf16), V((rows, columns), bf16), V((tall, side), bf16),
                V((2, 2, rows, 128), f32), V((2, 8, side), f32),
                V((2, models - 1, 2, rows, 128), f32), V((models - 1, 2, 8, side), f32),
                V((replicas,) + vectors.shape, f32), V((tall_n, 128), f32),
                DMA((3, units, 4)), DMA((3, units, 4)), DMA((3, units, 4)),
                DMA((3, units)), DMA((3, units)), DMA((3, units)), DMA((3, units)),
                DMA((3, models - 1)), DMA((3, models - 1)),
                DMA((replicas - 1,)), DMA((replicas,)),
                DMA((3, 2, 7)), DMA((3, 2, 7)), DMA((3, 2)), DMA((3,)),
            ],
            compiler_params=pltpu.CompilerParams(
                collective_id=0, has_side_effects=True, vmem_limit_bytes=67043328
            ),
        )(
            slope_gate.reshape(by_chip), slope_up.reshape(by_chip), slope_down[0],
            vectors, param_gate, param_up, param_down,
        )
        half_gate, half_up, half_down, next_gate, next_up, next_down, half_norm, next_norm = out
        return (
            half_gate, half_up, half_down, half_norm.reshape(-1),
            next_gate, next_up, next_down, next_norm.reshape(-1),
        )

    return run


def plain(
    slope_gate, slope_up, slope_down, slope_norm, param_gate, param_up, param_down, param_norm
):
    rate = lax.axis_size("replica") ** (-0.5)
    halves, nexts = [], []
    for slope, param, dim in (
        (slope_gate, param_gate, 0), (slope_up, param_up, 0), (slope_down, param_down, 1)
    ):
        mean = lax.psum_scatter(slope[0], "replica", scatter_dimension=dim, tiled=True) * rate
        own, size = lax.psum(
            (
                jnp.sum(param * param, axis=1 - dim, keepdims=True),
                jnp.sum(mean * mean, axis=1 - dim, keepdims=True),
            ),
            "model",
        )
        new = param - learn_rate * (mean * (jnp.sqrt(own) * lax.rsqrt(size + eps)))
        nexts.append(new)
        halves.append(lax.all_gather(new.astype(bf16), "replica", axis=dim, tiled=True))
    mean = lax.psum_scatter(slope_norm[0], "replica", scatter_dimension=0, tiled=True) * rate
    new = param_norm - learn_rate * mean
    nexts.append(new)
    halves.append(lax.all_gather(new.astype(bf16), "replica", axis=0, tiled=True))
    return (*halves, *nexts)


def solution(mesh):
    replicas, models = mesh.shape["replica"], mesh.shape["model"]
    body = fused(replicas, models) if replicas == 2 * 2 * 2 else plain
    matrix, turned = P("replica", "model"), P("model", "replica")
    return jax.shard_map(
        body,
        mesh=mesh,
        in_specs=(
            P("replica", None, "model"),
            P("replica", None, "model"),
            P("replica", "model", None),
            P("replica", None),
            matrix, matrix, turned, P("replica"),
        ),
        out_specs=(
            P(None, "model"), P(None, "model"), P("model", None), P(),
            matrix, matrix, turned, P("replica"),
        ),
        check_vma=False,
    )
```
